32 devices in a mesh: row: 8 (over z, core), col: 4 (over y, x).
Axes of the slice: x: 2, y: 2, z: 4, core: 2. Of those that a mesh axis runs over, the one named last changes fastest.
Arguments:
- gate_input: bfloat16 [2, 512, 53248], P(None, 'col', 'row'), may hold values from -6 to 6
- up_input: bfloat16 [2, 512, 53248], P(None, 'col', 'row'), may hold values from -6 to 6
- down_weight: bfloat16 [53248, 16384], P('row', 'col'), may hold values from -0.02734375 to 0.02734375
Outputs:
- mixed: bfloat16 [2, 512, 16384], P(None, 'row', 'col')
The draws below stay inside these ranges and needn't reach their ends.
All inputs are finite; a program needn't handle non-finite values.
Results may differ from the reference program's by a relative error of at most 0.0049.
Values may be sent and summed in bfloat16 or wider, within the bound.
A program may use at most 128 MiB of HBM per device.

```python
import jax
import jax.numpy as jnp

D = 16384
FF = 53248
SEQS = 2
MINISEQ = 512


def block_scale(key, dims, cuts, least, top_value):
    loudness = 1.0
    for axis_at, blocks in cuts:
        steps = jax.random.uniform(jax.random.fold_in(jax.random.fold_in(key, 6), axis_at), (blocks,), jnp.float32, least / len(cuts), top_value / len(cuts))
        loudness = loudness * jnp.repeat(jnp.exp(steps), dims[axis_at] // blocks).reshape((-1,) + (1,) * (len(dims) - 1 - axis_at))
    return loudness


def centred(own_key, shape, width, most, split=(), dtype=jnp.bfloat16):
    values = width * jax.random.normal(own_key, shape, jnp.float32)
    if split:
        values = values * block_scale(own_key, shape, split, -0.22, 0.18)
    return jnp.clip(values, -most, most).astype(dtype)


def setup_inputs(seed: int = 0) -> dict:
    key_of = jax.random.split(jax.random.key(seed), 4)
    gate_input = centred(key_of[0], (SEQS, MINISEQ, FF), 1.0, 6.0, ((1, 4), (2, 8)))
    up_input = centred(key_of[1], (SEQS, MINISEQ, FF), 1.0, 6.0, ((1, 4), (2, 8)))
    down_weight = centred(key_of[2], (FF, D), FF ** -0.5, 0.02734375, ((0, 8), (1, 4)))
    return dict(gate_input=gate_input, up_input=up_input, down_weight=down_weight)


def reference(gate_input, up_input, down_weight):
    hidden = (jax.nn.silu(gate_input.astype(jnp.float32)) * up_input.astype(jnp.float32)).astype(jnp.bfloat16)
    flat = hidden.reshape(SEQS * MINISEQ, FF)
    mixed = jnp.dot(flat, down_weight, preferred_element_type=jnp.float32)
    return mixed.astype(jnp.bfloat16).reshape(SEQS, MINISEQ, D)
```

```python
import functools

import jax
import jax.numpy as jnp
from jax import lax
from jax.sharding import PartitionSpec as P

PIECES = 4
PERMUTE = True


def gated_hidden(gate_part, up_part):
    product = jax.nn.silu(gate_part.astype(jnp.float32)) * up_part.astype(jnp.float32)
    return product.astype(jnp.bfloat16)


def gather_by_permutes(part, n):
    me = lax.axis_index("col")

    def swap(value, bit):
        return lax.ppermute(value, "col", [(i, i ^ bit) for i in range(n)])

    half = part.shape[0] // 2
    near = swap(part, 1)
    far = swap(part, 2)
    top = swap(near[:half], 2)
    low = swap(far[half:], 1)
    blocks = jnp.zeros((n,) + part.shape, part.dtype)
    blocks = lax.dynamic_update_slice(blocks, part[None], (me, 0, 0))
    blocks = lax.dynamic_update_slice(blocks, near[None], (me ^ 1, 0, 0))
    blocks = lax.dynamic_update_slice(blocks, far[None], (me ^ 2, 0, 0))
    blocks = lax.dynamic_update_slice(blocks, top[None], (me ^ 3, 0, 0))
    return lax.dynamic_update_slice(blocks, low[None], (me ^ 3, half, 0))


def body(cols, rows, gate_input, up_input, down_weight):
    hidden_units, width = down_weight.shape
    seqs, held, _ = gate_input.shape
    owned = held * cols // rows
    per_seq = max(PIECES // seqs, 1)
    step = owned // per_seq
    groups = held // owned
    outs = []
    for seq in range(seqs):
        seq_outs = []
        for piece in range(per_seq):
            def cut(a):
                a = a[seq].reshape(groups, owned, hidden_units)
                return a[:, piece * step:(piece + 1) * step].reshape(groups * step, hidden_units)
            part = gated_hidden(cut(gate_input), cut(up_input))
            if PERMUTE and cols == 4:
                flat = gather_by_permutes(part, cols).reshape(cols * groups * step, hidden_units)
            else:
                flat = lax.all_gather(part, "col", axis=0, tiled=True)
            partial_value = jnp.dot(flat, down_weight, preferred_element_type=jnp.float32).astype(jnp.bfloat16)
            seq_outs.append(lax.psum_scatter(partial_value, "row", scatter_dimension=0, tiled=True))
        outs.append(jnp.concatenate(seq_outs, axis=0) if per_seq > 1 else seq_outs[0])
    return jnp.stack(outs, axis=0)


def solution(mesh):
    return jax.shard_map(
        functools.partial(body, mesh.shape["col"], mesh.shape["row"]),
        mesh=mesh,
        in_specs=(P(None, "col", "row"), P(None, "col", "row"), P("row", "col")),
        out_specs=P(None, "row", "col"),
        check_vma=False,
    )
```
